8 devices in a mesh: dp: 1 (over z), ep: 8 (over y, x, core).
Axes of the slice: x: 2, y: 2, z: 1, core: 2. Of those that a mesh axis runs over, the one named last changes fastest.
Arguments:
- tok_x: bfloat16 [32768, 2304], P(('dp', 'ep'))
- route_ids: int32 [32768, 2], P(('dp', 'ep'))
- route_gate: float32 [32768, 2], P(('dp', 'ep'))
- w_in: bfloat16 [8, 2304, 5760], P('ep')
- w_out: bfloat16 [8, 5760, 2304], P('ep')
- shared_in: bfloat16 [2304, 5760], replicated
- shared_out: bfloat16 [5760, 2304], replicated
Outputs:
- output: bfloat16 [32768, 2304], P(('dp', 'ep'))
All inputs are finite; a program needn't handle non-finite values.
Results may differ from the reference program's by a relative error of at most 0.00522027.
Values are sent between devices in bfloat16 or wider.
A program may use at most 1 GiB of HBM per device.

```python
import jax
import jax.numpy as jnp
from jax import lax

D_MODEL = 2304
FF_EXPERT = 5760
FF_SHARED = 5760
EXPERTS = 8
TOP_K = 2
TOK_DEV = 4096
GROUP_DEV = 8
GROUP_TOK = GROUP_DEV * TOK_DEV
CAPACITY = GROUP_TOK * TOP_K // EXPERTS


def device_routing(dev_counts, rng_key):
    run_ends = jnp.cumsum(dev_counts)
    flat_ids = jnp.searchsorted(run_ends, jnp.arange(TOK_DEV * TOP_K), side='right')
    id_table = flat_ids.reshape(TOP_K, TOK_DEV).T
    key_order, key_turn = jax.random.split(rng_key)
    id_table = id_table[jax.random.permutation(key_order, TOK_DEV)]
    row_turn = jax.random.randint(key_turn, (TOK_DEV, 1), 0, TOP_K)
    col_index = (jnp.arange(TOP_K)[None, :] + row_turn) % TOP_K
    return jnp.take_along_axis(id_table, col_index, axis=1).astype(jnp.int32)


def draw_routing(rng_key):
    avg_load = TOK_DEV * TOP_K // EXPERTS
    spread = avg_load // 2
    half_experts = EXPERTS // 2
    key_bias, key_noise, key_perm, key_rows = jax.random.split(rng_key, 4)
    pair_bias = jax.random.randint(key_bias, (half_experts,), -spread, spread + 1)
    dev_noise = jax.random.randint(key_noise, (GROUP_DEV, half_experts), -spread, spread + 1)
    pair_shift = jnp.clip(pair_bias[None, :] + dev_noise, -avg_load, avg_load)
    forced = jnp.arange(half_experts)[None, :] == (jnp.arange(GROUP_DEV)[:, None] % half_experts)
    pair_shift = jnp.where(forced, avg_load, pair_shift)
    paired = jnp.stack([avg_load + pair_shift, avg_load - pair_shift], axis=-1).reshape(GROUP_DEV, EXPERTS)
    counts = paired[:, jax.random.permutation(key_perm, EXPERTS)]
    row_keys = jax.random.split(key_rows, GROUP_DEV)
    return jax.vmap(device_routing)(counts, row_keys).reshape(GROUP_TOK, TOP_K)


def setup_inputs(seed: int = 0, part: int = 0) -> dict:
    base_key = jax.random.key(seed)
    key_parts, key_weights = jax.random.split(base_key)
    part_key = jax.random.fold_in(key_parts, part)
    key_x, key_route, key_gate = jax.random.split(part_key, 3)
    key_w1, key_w2, key_s1, key_s2 = jax.random.split(key_weights, 4)
    tok_x = jax.random.normal(key_x, (GROUP_TOK, D_MODEL), jnp.float32).astype(jnp.bfloat16)
    route_ids = draw_routing(key_route)
    route_gate = jax.random.uniform(key_gate, (GROUP_TOK, TOP_K), jnp.float32, 0.5, 1.5) * TOP_K ** -0.5
    w_in = (jax.random.normal(key_w1, (EXPERTS, D_MODEL, FF_EXPERT), jnp.float32) * D_MODEL ** -0.5).astype(jnp.bfloat16)
    w_out = (jax.random.normal(key_w2, (EXPERTS, FF_EXPERT, D_MODEL), jnp.float32) * FF_EXPERT ** -0.5).astype(jnp.bfloat16)
    shared_in = (jax.random.normal(key_s1, (D_MODEL, FF_SHARED), jnp.float32) * D_MODEL ** -0.5).astype(jnp.bfloat16)
    shared_out = (jax.random.normal(key_s2, (FF_SHARED, D_MODEL), jnp.float32) * FF_SHARED ** -0.5).astype(jnp.bfloat16)
    return {'tok_x': tok_x, 'route_ids': route_ids, 'route_gate': route_gate, 'w_in': w_in, 'w_out': w_out, 'shared_in': shared_in, 'shared_out': shared_out}


def reference(tok_x, route_ids, route_gate, w_in, w_out, shared_in, shared_out):
    dev_ids = route_ids.reshape(GROUP_DEV, TOK_DEV * TOP_K)

    def count_step(offset, ids_dev):
        onehot = (ids_dev[:, None] == jnp.arange(EXPERTS)[None, :]).astype(jnp.int32)
        running = jnp.cumsum(onehot, axis=0)
        slot_dev = jnp.sum(running * onehot, axis=1) - 1 + offset[ids_dev]
        return offset + running[-1], slot_dev

    _, pair_slot = lax.scan(count_step, jnp.zeros((EXPERTS,), jnp.int32), dev_ids)
    pair_slot = pair_slot.reshape(-1)
    flat_ids = route_ids.reshape(-1)
    keep_pair = pair_slot < CAPACITY
    target = jnp.where(keep_pair, flat_ids * CAPACITY + pair_slot, EXPERTS * CAPACITY)
    pair_tok = jnp.arange(GROUP_TOK * TOP_K) // TOP_K
    tok_at = jnp.full((EXPERTS * CAPACITY,), GROUP_TOK, jnp.int32).at[target].set(pair_tok, mode='drop')
    gate_at = jnp.zeros((EXPERTS * CAPACITY,), jnp.float32).at[target].set(route_gate.reshape(-1), mode='drop')
    x_pad = jnp.concatenate([tok_x, jnp.zeros((1, D_MODEL), tok_x.dtype)], axis=0)

    def expert_step(moe_sum, inputs):
        tok_e, gate_e, w_first, w_second = inputs
        buffer = x_pad[tok_e]
        hidden = jax.nn.gelu(jnp.dot(buffer, w_first, preferred_element_type=jnp.float32)).astype(jnp.bfloat16)
        expert_out = jnp.dot(hidden, w_second, preferred_element_type=jnp.float32).astype(jnp.bfloat16)
        moe_sum = moe_sum.at[tok_e].add(gate_e[:, None] * expert_out.astype(jnp.float32), mode='drop')
        return moe_sum, None

    moe_sum, _ = lax.scan(expert_step, jnp.zeros((GROUP_TOK, D_MODEL), jnp.float32), (tok_at.reshape(EXPERTS, CAPACITY), gate_at.reshape(EXPERTS, CAPACITY), w_in, w_out))

    def shared_block(x_block):
        hidden = jax.nn.gelu(jnp.dot(x_block, shared_in, preferred_element_type=jnp.float32)).astype(jnp.bfloat16)
        return jnp.dot(hidden, shared_out, preferred_element_type=jnp.float32).astype(jnp.bfloat16)

    shared_y = lax.map(shared_block, tok_x.reshape(GROUP_DEV, TOK_DEV, D_MODEL)).reshape(GROUP_TOK, D_MODEL)
    return (tok_x.astype(jnp.float32) + shared_y.astype(jnp.float32) + moe_sum).astype(jnp.bfloat16)
```

```python
import functools

import jax
import jax.numpy as jnp
from jax import lax
from jax.experimental import pallas as pl
from jax.experimental.pallas import tpu as pltpu
from jax.sharding import PartitionSpec as P

C0 = 0.7978845608028654
C1 = C0 * 0.044715

def gelu(a):
    half = 0.5 * a
    return half + half * jnp.tanh(a * (C0 + C1 * (a * a)))

def cuts(total, step):
    return [(s, min(step, total - s)) for s in range(0, total, step)]

def ffn_kernel(step_h, step_o, nv_ref, bi_ref, x_ref, win_hbm, wout_hbm, o_ref, win_v, wout_v, h_v, sem):
    s = pl.program_id(0)
    ff = win_v.shape[1]
    width = wout_v.shape[1]
    cin = pltpu.make_async_copy(win_hbm, win_v, sem.at[0])
    cout = pltpu.make_async_copy(wout_hbm, wout_v, sem.at[1])

    @pl.when(s == 0)
    def _():
        cin.start()
        cout.start()
        cin.wait()

    @pl.when(s < nv_ref[0])
    def _():
        for st, sz in cuts(ff, step_h):
            a = jnp.dot(x_ref[...], win_v[:, st:st + sz], preferred_element_type=jnp.float32)
            h_v[:, st:st + sz] = gelu(a).astype(jnp.bfloat16)

    @pl.when(s == 0)
    def _():
        cout.wait()

    @pl.when(s < nv_ref[0])
    def _():
        for st, sz in cuts(width, step_o):
            o_ref[:, st:st + sz] = jnp.dot(h_v[...], wout_v[:, st:st + sz], preferred_element_type=jnp.float32).astype(jnp.bfloat16)

def ffn(x, nv, bi, w_in, w_out, bm, step_h=1280, step_o=768):
    rows, width = x.shape
    ff = w_in.shape[1]
    nb = rows // bm
    def imap(s, nv_ref, bi_ref):
        return (bi_ref[jnp.minimum(s, jnp.maximum(nv_ref[0] - 1, 0))], 0)
    return pl.pallas_call(
        functools.partial(ffn_kernel, step_h, step_o),
        grid_spec=pltpu.PrefetchScalarGridSpec(
            num_scalar_prefetch=2, grid=(nb,),
            in_specs=[pl.BlockSpec((bm, width), imap), pl.BlockSpec(memory_space=pl.ANY), pl.BlockSpec(memory_space=pl.ANY)],
            out_specs=pl.BlockSpec((bm, width), imap),
            scratch_shapes=[pltpu.VMEM((width, ff), jnp.bfloat16), pltpu.VMEM((ff, width), jnp.bfloat16), pltpu.VMEM((bm, ff), jnp.bfloat16), pltpu.SemaphoreType.DMA((2,))]),
        out_shape=jax.ShapeDtypeStruct((rows, width), jnp.bfloat16),
        compiler_params=pltpu.CompilerParams(dimension_semantics=("arbitrary",), vmem_limit_bytes=67043328),
        cost_estimate=pl.CostEstimate(flops=4 * rows * width * ff, bytes_accessed=4 * rows * width + 4 * width * ff, transcendentals=rows * ff),
        name="ffn")(nv, bi, x, w_in, w_out)


ROWS_BLOCK = 128
RANK_CHUNK = 512


def valid_blocks(seg_rows, seg_len, bm):
    starts = jnp.arange(seg_len // bm, dtype=jnp.int32) * bm
    valid = (starts[None, :] < seg_rows[:, None]).reshape(-1).astype(jnp.int32)
    place = jnp.cumsum(valid) - 1
    number = jnp.arange(valid.shape[0], dtype=jnp.int32)
    hit = (place[None, :] == number[:, None]) & (valid[None, :] > 0)
    return jnp.sum(valid).reshape(1), jnp.sum(jnp.where(hit, number[None, :], 0), axis=1)


def solution(mesh):
    group_size = mesh.shape['ep']

    def device_layer(tok_x, route_ids, route_gate, w_in, w_out, shared_in, shared_out):
        tokens, width = tok_x.shape
        top_k = route_ids.shape[1]
        experts = group_size
        capacity = tokens * group_size * top_k // experts
        local_cap = 2 * tokens * top_k // experts
        me = lax.axis_index('ep')
        flat_ids = route_ids.reshape(-1)
        onehot = (flat_ids[:, None] == jnp.arange(experts, dtype=jnp.int32)[None, :]).astype(jnp.int32)
        running = jnp.cumsum(onehot, axis=0)
        rank = jnp.sum(running * onehot, axis=1) - 1
        counts = running[-1]
        all_counts = lax.all_gather(counts, 'ep')
        offset = jnp.cumsum(all_counts, axis=0) - all_counts
        kept = jnp.clip(capacity - offset, 0, all_counts)
        kept_home = jnp.sum(onehot * lax.dynamic_index_in_dim(kept, me, 0, keepdims=True), axis=1)
        kept_here = lax.dynamic_index_in_dim(kept, me, 1, keepdims=False)
        keep_pair = (rank < kept_home).reshape(tokens, top_k)

        chunk = RANK_CHUNK
        n_chunks = local_cap // chunk
        chunk_rows = experts * chunk
        pair_chunk = rank // chunk
        pair_at = flat_ids * chunk + rank % chunk
        pair_tok = jnp.arange(tokens * top_k, dtype=jnp.int32) // top_k
        send_tok = jnp.zeros((n_chunks * chunk_rows,), jnp.int32).at[pair_chunk * chunk_rows + pair_at].set(pair_tok)
        pair_chunk = pair_chunk.reshape(tokens, top_k)
        pair_at = pair_at.reshape(tokens, top_k)

        recv = []
        for q in range(n_chunks):
            rows = tok_x[send_tok[q * chunk_rows:(q + 1) * chunk_rows]].reshape(experts, chunk, width)
            recv.append(lax.all_to_all(rows, 'ep', 0, 0, tiled=True))
        every = tokens // ROWS_BLOCK
        shared_y = ffn(tok_x, jnp.full((1,), every, jnp.int32), jnp.arange(every, dtype=jnp.int32), shared_in, shared_out, ROWS_BLOCK)
        home = []
        for q in range(n_chunks):
            count, blocks = valid_blocks(jnp.clip(kept_here - q * chunk, 0, chunk), chunk, ROWS_BLOCK)
            out = ffn(recv[q].reshape(chunk_rows, width), count, blocks, w_in[0], w_out[0], ROWS_BLOCK)
            home.append(lax.all_to_all(out.reshape(experts, chunk, width), 'ep', 0, 0, tiled=True).reshape(chunk_rows, width))
        total = tok_x.astype(jnp.float32) + shared_y.astype(jnp.float32)
        for q in range(n_chunks):
            for j in range(top_k):
                take = (pair_chunk[:, j] == q) & keep_pair[:, j]
                rows = home[q][jnp.where(take, pair_at[:, j], 0)]
                total = total + jnp.where(take[:, None], route_gate[:, j:j + 1] * rows.astype(jnp.float32), 0.0)
        return total.astype(jnp.bfloat16)

    row_spec = P(('dp', 'ep'), None)
    expert_spec = P('ep', None, None)
    whole_spec = P(None, None)
    return jax.shard_map(device_layer, mesh=mesh, in_specs=(row_spec, row_spec, row_spec, expert_spec, expert_spec, whole_spec, whole_spec), out_specs=row_spec, check_vma=False)
```

```python
import functools

import jax
import jax.numpy as jnp
from jax import lax
from jax.experimental import pallas as pl
from jax.experimental.pallas import tpu as pltpu
from jax.sharding import PartitionSpec as P


C0 = 0.7978845608028654
C1 = C0 * 0.044715
BLOCK = 128
VMEM_BYTES = 67043328
GROUPS = ((0, 1), (2, 4), (3, 5), (6, 7))


def gelu(a):
    half = 0.5 * a
    return half + half * jnp.tanh(a * (C0 + C1 * (a * a)))


def cuts(total, step):
    return [(s, min(step, total - s)) for s in range(0, total, step)]


def ffn_kernel(parts, base, count_ref, *refs):
    xs, (win_hbm, wout_hbm), outs = refs[:parts], refs[parts:parts + 2], refs[parts + 2:2 * parts + 2]
    win_v, wout_v, h_v, x_v, o_v, wsem, xsem, osem = refs[2 * parts + 2:]
    ff, width = wout_v.shape
    ends = []
    total = 0
    for k in range(parts):
        total = total + count_ref[k]
        ends.append(total)
    load_in = pltpu.make_async_copy(win_hbm, win_v, wsem.at[0])
    load_out = pltpu.make_async_copy(wout_hbm, wout_v, wsem.at[1])
    load_in.start()
    load_out.start()

    def each_part(i, act):
        for k in range(parts):
            first = ends[k - 1] if k else 0

            @pl.when((i >= first) & (i < ends[k]))
            def _():
                act(k, pl.multiple_of((i - first) * BLOCK, BLOCK))

    def fetch(i, slot):
        each_part(i, lambda k, row: pltpu.make_async_copy(xs[k].at[pl.ds(base + row, BLOCK)], x_v.at[slot], xsem.at[slot]).start())

    def put(i, slot):
        each_part(i, lambda k, row: pltpu.make_async_copy(o_v.at[slot], outs[k].at[pl.ds(row, BLOCK)], osem.at[slot]).start())

    def wait_fetch(slot):
        pltpu.make_async_copy(xs[0].at[pl.ds(0, BLOCK)], x_v.at[slot], xsem.at[slot]).wait()

    def wait_put(slot):
        pltpu.make_async_copy(o_v.at[slot], outs[0].at[pl.ds(0, BLOCK)], osem.at[slot]).wait()

    fetch(0, 0)
    load_in.wait()

    @pl.when(total == 0)
    def _():
        load_out.wait()

    def step(i, carry):
        slot = lax.rem(i, 2)
        fetch(i + 1, 1 - slot)
        wait_fetch(slot)
        for st, sz in cuts(ff, 1280):
            a = jnp.dot(x_v[slot], win_v[:, st:st + sz], preferred_element_type=jnp.float32)
            h_v[:, st:st + sz] = gelu(a).astype(jnp.bfloat16)

        @pl.when(i == 0)
        def _():
            load_out.wait()

        @pl.when(i >= 2)
        def _():
            wait_put(slot)

        for st, sz in cuts(width, 768):
            o_v[slot, :, st:st + sz] = jnp.dot(h_v[...], wout_v[:, st:st + sz], preferred_element_type=jnp.float32).astype(jnp.bfloat16)
        put(i, slot)
        return carry

    lax.fori_loop(0, total, step, 0)

    @pl.when(total >= 1)
    def _():
        wait_put(lax.rem(total - 1, 2))

    @pl.when(total >= 2)
    def _():
        wait_put(lax.rem(total, 2))


def ffn(xs, counts, w_in, w_out, name, base=0, rows=None):
    parts = len(xs)
    width, ff = w_in.shape
    rows = rows or xs[0].shape[0]
    hbm = pl.BlockSpec(memory_space=pl.ANY)
    return pl.pallas_call(
        functools.partial(ffn_kernel, parts, base),
        in_specs=[pl.BlockSpec(memory_space=pltpu.SMEM)] + [hbm] * (parts + 2),
        out_specs=[hbm] * parts,
        out_shape=[jax.ShapeDtypeStruct((rows, width), x.dtype) for x in xs],
        scratch_shapes=[
            pltpu.VMEM((width, ff), jnp.bfloat16), pltpu.VMEM((ff, width), jnp.bfloat16), pltpu.VMEM((BLOCK, ff), jnp.bfloat16),
            pltpu.VMEM((2, BLOCK, width), jnp.bfloat16), pltpu.VMEM((2, BLOCK, width), jnp.bfloat16),
            pltpu.SemaphoreType.DMA((2,)), pltpu.SemaphoreType.DMA((2,)), pltpu.SemaphoreType.DMA((2,))],
        compiler_params=pltpu.CompilerParams(vmem_limit_bytes=VMEM_BYTES),
        cost_estimate=pl.CostEstimate(flops=2 * parts * rows * width * ff, bytes_accessed=4 * parts * rows * width + 4 * width * ff, transcendentals=0),
        name=name)(counts, *xs, w_in, w_out)


def add_kernel(parts, starts, final, count_ref, pair_ref, gate_ref, *refs):
    n_in = starts + 1
    ins, tables, (out,) = refs[:n_in], refs[n_in:n_in + parts], refs[n_in + parts:n_in + parts + 1]
    acc, rows_v, wide, buf_a, buf_b, rsem, asem, bsem = refs[n_in + parts + 1:]
    tokens, width = acc.shape
    block = rows_v.shape[1]
    cap = tables[0].shape[0]
    io = buf_a.shape[1]
    halves = cuts(width, (width // 256) * 128 or width)

    if starts:
        per = tokens // starts // io
        n_io = tokens // io

        def load(i):
            a = pltpu.make_async_copy(ins[0].at[pl.ds(i * io, io)], buf_a.at[i % 2], asem.at[i % 2])
            b = pltpu.make_async_copy(ins[1 + i // per].at[pl.ds((i % per) * io, io)], buf_b.at[i % 2], bsem.at[i % 2])
            return a, b

        for c in load(0):
            c.start()
        for i in range(n_io):
            if i + 1 < n_io:
                for c in load(i + 1):
                    c.start()
            for c in load(i):
                c.wait()
            acc[pl.ds(i * io, io), :] = buf_a[i % 2].astype(jnp.float32) + buf_b[i % 2].astype(jnp.float32)
    else:
        whole = pltpu.make_async_copy(ins[0], acc, asem.at[0])
        whole.start()
        whole.wait()

    for k in range(parts):
        number = count_ref[k]
        blocks = (number + block - 1) // block

        def fetch(b, slot, k=k):
            return pltpu.make_async_copy(tables[k].at[pl.ds(pl.multiple_of(b * block, block), block)], rows_v.at[slot], rsem.at[slot])

        @pl.when(blocks > 0)
        def _(fetch=fetch):
            fetch(0, 0).start()

        def one_block(b, carry, k=k, fetch=fetch, blocks=blocks, number=number):
            slot = lax.rem(b, 2)

            @pl.when(b + 1 < blocks)
            def _():
                fetch(b + 1, 1 - slot).start()

            fetch(b, slot).wait()
            wide[...] = rows_v[slot].astype(jnp.float32)
            here = jnp.minimum(block, number - b * block)

            def some_rows(r, unroll):
                pairs = [pair_ref[k * cap + b * block + r + u] for u in range(unroll)]
                toks = [lax.shift_right_logical(p, 1) for p in pairs]
                gates = [gate_ref[p] for p in pairs]
                for st, sz in halves:
                    sums = [acc[pl.ds(t, 1), st:st + sz] + g * wide[pl.ds(r + u, 1), st:st + sz] for u, (t, g) in enumerate(zip(toks, gates))]
                    for t, s in zip(toks, sums):
                        acc[pl.ds(t, 1), st:st + sz] = s

            def four(q, c):
                some_rows(q * 4, 4)
                return c

            def single(r, c):
                some_rows(r, 1)
                return c

            lax.fori_loop(0, here // 4, four, 0)
            lax.fori_loop(here // 4 * 4, here, single, 0)
            return carry

        lax.fori_loop(0, blocks, one_block, 0)

    if final:
        n_io = tokens // io

        def store(i):
            return pltpu.make_async_copy(buf_a.at[i % 2], out.at[pl.ds(i * io, io)], asem.at[i % 2])

        for i in range(n_io):
            if i >= 2:
                store(i - 2).wait()
            buf_a[i % 2] = acc[pl.ds(i * io, io), :].astype(jnp.bfloat16)
            store(i).start()
        for i in range(max(n_io - 2, 0), n_io):
            store(i).wait()
    else:
        whole = pltpu.make_async_copy(acc, out, asem.at[0])
        whole.start()
        whole.wait()


def add_rows(ins, tables, counts, pairs, gates, tokens, final, name, io=256):
    width = tables[0].shape[1]
    starts = len(ins) - 1
    hbm = pl.BlockSpec(memory_space=pl.ANY)
    smem = pl.BlockSpec(memory_space=pltpu.SMEM)
    return pl.pallas_call(
        functools.partial(add_kernel, len(tables), starts, final),
        in_specs=[smem] * 3 + [hbm] * (len(ins) + len(tables)),
        out_specs=hbm,
        out_shape=jax.ShapeDtypeStruct((tokens, width), jnp.bfloat16 if final else jnp.float32),
        scratch_shapes=[
            pltpu.VMEM((tokens, width), jnp.float32), pltpu.VMEM((2, BLOCK, width), jnp.bfloat16), pltpu.VMEM((BLOCK, width), jnp.float32),
            pltpu.VMEM((2, io, width), jnp.bfloat16), pltpu.VMEM((2, io, width), jnp.bfloat16),
            pltpu.SemaphoreType.DMA((2,)), pltpu.SemaphoreType.DMA((2,)), pltpu.SemaphoreType.DMA((2,))],
        compiler_params=pltpu.CompilerParams(vmem_limit_bytes=VMEM_BYTES),
        cost_estimate=pl.CostEstimate(flops=60 * 1000 * 1000 * 1000, bytes_accessed=6 * tokens * width, transcendentals=0),
        name=name)(counts, pairs, gates, *ins, *tables)


def after(value, *others):
    return lax.optimization_barrier((value,) + others)[0]


def solution(mesh):
    group_size = mesh.shape['ep']

    def swap(x, bits):
        return lax.ppermute(x, 'ep', [(i, i ^ bits) for i in range(group_size)])

    def device_layer(tok_x, route_ids, route_gate, w_in, w_out, shared_in, shared_out):
        tokens, width = tok_x.shape
        top_k = route_ids.shape[1]
        experts = group_size
        capacity = tokens * group_size * top_k // experts
        local_cap = 2 * tokens * top_k // experts
        half = tokens // 2
        me = lax.axis_index('ep')
        partner = jnp.bitwise_xor(me, jnp.arange(experts, dtype=jnp.int32))

        flat_ids = route_ids.reshape(-1)
        onehot = (flat_ids[:, None] == jnp.arange(experts, dtype=jnp.int32)[None, :]).astype(jnp.int32)
        running = jnp.cumsum(onehot, axis=0)
        rank = jnp.sum(running * onehot, axis=1) - 1
        all_counts = lax.all_gather(running[-1], 'ep')
        offset = jnp.cumsum(all_counts, axis=0) - all_counts
        kept = jnp.clip(capacity - offset, 0, all_counts)
        relation = jnp.arange(experts, dtype=jnp.int32)
        kept_out = lax.dynamic_index_in_dim(kept, me, 0, keepdims=False)[partner]
        kept_here = lax.dynamic_index_in_dim(kept, me, 1, keepdims=False)[partner]
        pair_number = jnp.arange(tokens * top_k, dtype=jnp.int32)
        lists = jnp.zeros((experts * local_cap,), jnp.int32).at[flat_ids * local_cap + rank].set(pair_number)
        lists = lists.reshape(experts, local_cap)
        got_lists = lax.all_to_all(lists, 'ep', 0, 0, tiled=True)
        here_toks = got_lists[partner] // top_k
        home_pairs = lists[partner]
        block_counts = (kept_here + BLOCK - 1) // BLOCK
        gates = route_gate.reshape(-1)

        first_x = after(tok_x, got_lists, all_counts)
        from_core = swap(tok_x, 1)
        from_x = swap(first_x, 2)
        from_y = swap(first_x, 4)

        shared_blocks = jnp.full((1,), half // BLOCK, jnp.int32)
        shared_a, = ffn([tok_x], after(shared_blocks, got_lists), shared_in, shared_out, 'shared_ffn', 0, half)

        home = [None] * experts

        def expert(group, sources, previous):
            rows = [x[here_toks[s]] for x, s in zip(sources, group)]
            counts = after(jnp.stack([block_counts[s] for s in group]), previous)
            outs = ffn(rows, counts, w_in[0], w_out[0], 'expert_ffn')
            for s, out in zip(group, outs):
                home[s] = swap(out, s) if s else out
            return outs[0]

        last = expert(GROUPS[0], (tok_x, from_core), shared_a)
        from_x, from_y = after(from_x, last), after(from_y, last)
        diag_a = swap(from_x[:half], 4)
        diag_b = swap(from_y[half:], 2)
        core_x = swap(from_x, 1)
        core_y = swap(from_y, 1)
        last = expert(GROUPS[1], (from_x, from_y), last)
        last = expert(GROUPS[2], (core_x, core_y), last)
        diag = jnp.concatenate([diag_a, diag_b], axis=0)
        core_diag = swap(diag, 1)
        last = expert(GROUPS[3], (diag, core_diag), last)
        shared_b, = ffn([tok_x], after(shared_blocks, last), shared_in, shared_out, 'shared_ffn_b', half, half)

        early = [s for group in GROUPS[:3] for s in group]
        late = list(GROUPS[3])
        total = add_rows([tok_x, shared_a, shared_b], [home[s] for s in early], jnp.stack([kept_out[s] for s in early]),
                         jnp.concatenate([home_pairs[s] for s in early]), gates, tokens, False, 'add_early')
        return add_rows([total], [home[s] for s in late], jnp.stack([kept_out[s] for s in late]),
                        jnp.concatenate([home_pairs[s] for s in late]), gates, tokens, True, 'add_late')

    row_spec = P(('dp', 'ep'), None)
    expert_spec = P('ep', None, None)
    whole_spec = P(None, None)
    return jax.shard_map(device_layer, mesh=mesh, in_specs=(row_spec, row_spec, row_spec, expert_spec, expert_spec, whole_spec, whole_spec), out_specs=row_spec, check_vma=False)
```

```python
import functools

import jax
import jax.numpy as jnp
from jax import lax
from jax.experimental import pallas as pl
from jax.experimental.pallas import tpu as pltpu
from jax.sharding import PartitionSpec as P


C0 = 0.7978845608028654
C1 = C0 * 0.044715
BLOCK = 256
ADD_BLOCK = 128
VMEM_BYTES = 67043328


def gelu(a):
    half = 0.5 * a
    return half + half * jnp.tanh(a * (C0 + C1 * (a * a)))


def cuts(total, step):
    return [(s, min(step, total - s)) for s in range(0, total, step)]


def ffn_kernel(parts, count_ref, *refs):
    xs, (win_hbm, wout_hbm), outs = refs[:parts], refs[parts:parts + 2], refs[parts + 2:2 * parts + 2]
    win_v, wout_v, h_v, x_v, o_v, wsem, xsem, osem = refs[2 * parts + 2:]
    ff, width = wout_v.shape
    ends = []
    total = 0
    for k in range(parts):
        total = total + count_ref[k]
        ends.append(total)
    load_in = pltpu.make_async_copy(win_hbm, win_v, wsem.at[0])
    load_out = pltpu.make_async_copy(wout_hbm, wout_v, wsem.at[1])
    load_in.start()
    load_out.start()

    def each_part(i, act):
        for k in range(parts):
            first = ends[k - 1] if k else 0

            @pl.when((i >= first) & (i < ends[k]))
            def _():
                act(k, pl.multiple_of((i - first) * BLOCK, BLOCK))

    def fetch(i, slot):
        each_part(i, lambda k, row: pltpu.make_async_copy(xs[k].at[pl.ds(row, BLOCK)], x_v.at[slot], xsem.at[slot]).start())

    def put(i, slot):
        each_part(i, lambda k, row: pltpu.make_async_copy(o_v.at[slot], outs[k].at[pl.ds(row, BLOCK)], osem.at[slot]).start())

    def wait_fetch(slot):
        pltpu.make_async_copy(xs[0].at[pl.ds(0, BLOCK)], x_v.at[slot], xsem.at[slot]).wait()

    def wait_put(slot):
        pltpu.make_async_copy(o_v.at[slot], outs[0].at[pl.ds(0, BLOCK)], osem.at[slot]).wait()

    fetch(0, 0)
    load_in.wait()

    @pl.when(total == 0)
    def _():
        load_out.wait()

    def step(i, carry):
        slot = lax.rem(i, 2)
        fetch(i + 1, 1 - slot)
        wait_fetch(slot)
        for st, sz in cuts(ff, 1280):
            a = jnp.dot(x_v[slot], win_v[:, st:st + sz], preferred_element_type=jnp.float32)
            h_v[:, st:st + sz] = gelu(a).astype(jnp.bfloat16)

        @pl.when(i == 0)
        def _():
            load_out.wait()

        @pl.when(i >= 2)
        def _():
            wait_put(slot)

        for st, sz in cuts(width, 768):
            o_v[slot, :, st:st + sz] = jnp.dot(h_v[...], wout_v[:, st:st + sz], preferred_element_type=jnp.float32).astype(jnp.bfloat16)
        put(i, slot)
        return carry

    lax.fori_loop(0, total, step, 0)

    @pl.when(total >= 1)
    def _():
        wait_put(lax.rem(total - 1, 2))

    @pl.when(total >= 2)
    def _():
        wait_put(lax.rem(total, 2))


def ffn(xs, counts, w_in, w_out):
    parts = len(xs)
    width, ff = w_in.shape
    rows = xs[0].shape[0]
    hbm = pl.BlockSpec(memory_space=pl.ANY)
    return pl.pallas_call(
        functools.partial(ffn_kernel, parts),
        in_specs=[pl.BlockSpec(memory_space=pltpu.SMEM)] + [hbm] * (parts + 2),
        out_specs=[hbm] * parts,
        out_shape=[jax.ShapeDtypeStruct((rows, width), x.dtype) for x in xs],
        scratch_shapes=[
            pltpu.VMEM((width, ff), jnp.bfloat16), pltpu.VMEM((ff, width), jnp.bfloat16), pltpu.VMEM((BLOCK, ff), jnp.bfloat16),
            pltpu.VMEM((2, BLOCK, width), jnp.bfloat16), pltpu.VMEM((2, BLOCK, width), jnp.bfloat16),
            pltpu.SemaphoreType.DMA((2,)), pltpu.SemaphoreType.DMA((2,)), pltpu.SemaphoreType.DMA((2,))],
        compiler_params=pltpu.CompilerParams(vmem_limit_bytes=VMEM_BYTES),
        cost_estimate=pl.CostEstimate(flops=2 * parts * rows * width * ff, bytes_accessed=4 * parts * rows * width + 4 * width * ff, transcendentals=0))(counts, *xs, w_in, w_out)


def add_kernel(parts, starts, final, count_ref, pair_ref, gate_ref, *refs):
    n_in = starts + 1
    ins, tables, (out,) = refs[:n_in], refs[n_in:n_in + parts], refs[n_in + parts:n_in + parts + 1]
    acc, rows_v, wide, buf_a, buf_b, rsem, asem, bsem = refs[n_in + parts + 1:]
    tokens, width = acc.shape
    block = rows_v.shape[1]
    cap = tables[0].shape[0]
    io = buf_a.shape[1]
    halves = cuts(width, (width // 256) * 128 or width)

    if starts:
        per = tokens // starts // io
        n_io = tokens // io

        def load(i):
            a = pltpu.make_async_copy(ins[0].at[pl.ds(i * io, io)], buf_a.at[i % 2], asem.at[i % 2])
            b = pltpu.make_async_copy(ins[1 + i // per].at[pl.ds((i % per) * io, io)], buf_b.at[i % 2], bsem.at[i % 2])
            return a, b

        for c in load(0):
            c.start()
        for i in range(n_io):
            if i + 1 < n_io:
                for c in load(i + 1):
                    c.start()
            for c in load(i):
                c.wait()
            acc[pl.ds(i * io, io), :] = buf_a[i % 2].astype(jnp.float32) + buf_b[i % 2].astype(jnp.float32)
    else:
        whole = pltpu.make_async_copy(ins[0], acc, asem.at[0])
        whole.start()
        whole.wait()

    for k in range(parts):
        number = count_ref[k]
        blocks = (number + block - 1) // block

        def fetch(b, slot, k=k):
            return pltpu.make_async_copy(tables[k].at[pl.ds(pl.multiple_of(b * block, block), block)], rows_v.at[slot], rsem.at[slot])

        @pl.when(blocks > 0)
        def _(fetch=fetch):
            fetch(0, 0).start()

        def one_block(b, carry, k=k, fetch=fetch, blocks=blocks, number=number):
            slot = lax.rem(b, 2)

            @pl.when(b + 1 < blocks)
            def _():
                fetch(b + 1, 1 - slot).start()

            fetch(b, slot).wait()
            wide[...] = rows_v[slot].astype(jnp.float32)
            here = jnp.minimum(block, number - b * block)

            def some_rows(r, unroll):
                pairs = [pair_ref[k * cap + b * block + r + u] for u in range(unroll)]
                toks = [lax.shift_right_logical(p, 1) for p in pairs]
                gates = [gate_ref[p] for p in pairs]
                for st, sz in halves:
                    sums = [acc[pl.ds(t, 1), st:st + sz] + g * wide[pl.ds(r + u, 1), st:st + sz] for u, (t, g) in enumerate(zip(toks, gates))]
                    for t, s in zip(toks, sums):
                        acc[pl.ds(t, 1), st:st + sz] = s

            def four(q, c):
                some_rows(q * 4, 4)
                return c

            def single(r, c):
                some_rows(r, 1)
                return c

            lax.fori_loop(0, here // 4, four, 0)
            lax.fori_loop(here // 4 * 4, here, single, 0)
            return carry

        lax.fori_loop(0, blocks, one_block, 0)

    if final:
        n_io = tokens // io

        def store(i):
            return pltpu.make_async_copy(buf_a.at[i % 2], out.at[pl.ds(i * io, io)], asem.at[i % 2])

        for i in range(n_io):
            if i >= 2:
                store(i - 2).wait()
            buf_a[i % 2] = acc[pl.ds(i * io, io), :].astype(jnp.bfloat16)
            store(i).start()
        for i in range(max(n_io - 2, 0), n_io):
            store(i).wait()
    else:
        whole = pltpu.make_async_copy(acc, out, asem.at[0])
        whole.start()
        whole.wait()


def add_rows(ins, tables, counts, pairs, gates, tokens, final, io=256):
    width = tables[0].shape[1]
    starts = len(ins) - 1
    hbm = pl.BlockSpec(memory_space=pl.ANY)
    smem = pl.BlockSpec(memory_space=pltpu.SMEM)
    return pl.pallas_call(
        functools.partial(add_kernel, len(tables), starts, final),
        in_specs=[smem] * 3 + [hbm] * (len(ins) + len(tables)),
        out_specs=hbm,
        out_shape=jax.ShapeDtypeStruct((tokens, width), jnp.bfloat16 if final else jnp.float32),
        scratch_shapes=[
            pltpu.VMEM((tokens, width), jnp.float32), pltpu.VMEM((2, ADD_BLOCK, width), jnp.bfloat16), pltpu.VMEM((ADD_BLOCK, width), jnp.float32),
            pltpu.VMEM((2, io, width), jnp.bfloat16), pltpu.VMEM((2, io, width), jnp.bfloat16),
            pltpu.SemaphoreType.DMA((2,)), pltpu.SemaphoreType.DMA((2,)), pltpu.SemaphoreType.DMA((2,))],
        compiler_params=pltpu.CompilerParams(vmem_limit_bytes=VMEM_BYTES),
        cost_estimate=pl.CostEstimate(flops=60 * 1000 * 1000 * 1000, bytes_accessed=6 * tokens * width, transcendentals=0))(counts, pairs, gates, *ins, *tables)


def after(value, *others):
    return lax.optimization_barrier((value,) + others)[0]


def solution(mesh):
    group_size = mesh.shape['ep']

    def swap(x, bits):
        return lax.ppermute(x, 'ep', [(i, i ^ bits) for i in range(group_size)])

    def layer(tok_x, route_ids, route_gate, w_in, w_out, shared_in, shared_out):
        tokens, _ = tok_x.shape
        top_k = route_ids.shape[1]
        experts = group_size
        capacity = tokens * group_size * top_k // experts
        local_cap = 2 * tokens * top_k // experts
        half = tokens // 2
        me = lax.axis_index('ep')
        partner = jnp.bitwise_xor(me, jnp.arange(experts, dtype=jnp.int32))

        flat_ids = route_ids.reshape(-1)
        onehot = (flat_ids[:, None] == jnp.arange(experts, dtype=jnp.int32)[None, :]).astype(jnp.int32)
        running = jnp.cumsum(onehot, axis=0)
        rank = jnp.sum(running * onehot, axis=1) - 1
        counts = running[-1]
        pair_number = jnp.arange(tokens * top_k, dtype=jnp.int32)
        lists = jnp.zeros((experts * local_cap,), jnp.int32).at[flat_ids * local_cap + rank].set(pair_number)
        lists = lists.reshape(experts, local_cap)
        notes = jnp.concatenate([lists, jnp.broadcast_to(jnp.pad(counts, (0, 128 - experts))[None, :], (experts, 128))], axis=1)
        notes = lax.all_to_all(notes, 'ep', 0, 0, tiled=True)
        all_counts = notes[:, local_cap:local_cap + experts]
        offset = jnp.cumsum(all_counts, axis=0) - all_counts
        kept = jnp.clip(capacity - offset, 0, all_counts)
        kept_out = lax.dynamic_index_in_dim(kept, me, 0, keepdims=False)[partner]
        kept_here = lax.dynamic_index_in_dim(kept, me, 1, keepdims=False)[partner]
        here_toks = notes[partner, :local_cap] // top_k
        home_pairs = lists[partner]
        block_counts = (kept_here + BLOCK - 1) // BLOCK
        gates = route_gate.reshape(-1)

        from_core = swap(tok_x, 1)
        from_x = swap(tok_x, 2)
        from_y = swap(tok_x, 4)

        every = jnp.full((1,), tokens // BLOCK, jnp.int32)
        shared_y, = ffn([tok_x], every, shared_in, shared_out)

        home = [None] * experts

        def expert(group, sources, previous):
            toks = after(here_toks, previous) if group == (0, 1) else here_toks
            rows = [x[toks[s]] for x, s in zip(sources, group)]
            number = after(jnp.stack([block_counts[s] for s in group]), previous)
            outs = ffn(rows, number, w_in[0], w_out[0])
            for s, out in zip(group, outs):
                home[s] = swap(out, s) if s else out
            return outs[0]

        part_x, part_y = from_x[:half], from_y[half:]
        diag_a = swap(part_x, 4)
        diag_b = swap(part_y, 2)
        core_x = swap(from_x, 1)
        core_y = swap(from_y, 1)
        last = expert((2, 4), (from_x, from_y), shared_y)
        diag_a, diag_b = after(diag_a, last), after(diag_b, last)
        diag = jnp.concatenate([diag_a, diag_b], axis=0)
        core_diag = swap(diag, 1)
        last = expert((3, 5), (core_x, core_y), last)
        last = expert((6,), (diag,), last)
        last = expert((7,), (core_diag,), last)
        last = expert((0, 1), (tok_x, from_core), last)

        def add(ins, classes, final):
            return add_rows(ins, [home[s] for s in classes], jnp.stack([kept_out[s] for s in classes]),
                            jnp.concatenate([home_pairs[s] for s in classes]), gates, tokens, final)

        total = add([tok_x, shared_y], (2, 4, 3, 5, 0, 1, 6), False)
        return add([total], (7,), True)

    row_spec = P(('dp', 'ep'), None)
    expert_spec = P('ep', None, None)
    whole_spec = P(None, None)
    return jax.shard_map(layer, mesh=mesh, in_specs=(row_spec, row_spec, row_spec, expert_spec, expert_spec, whole_spec, whole_spec), out_specs=row_spec, check_vma=False)
```

```python
import functools

import jax
import jax.numpy as jnp
from jax import lax
from jax.experimental import pallas as pl
from jax.experimental.pallas import tpu as pltpu
from jax.sharding import PartitionSpec as P


C0 = 0.7978845608028654
C1 = C0 * 0.044715
BLOCK = 256
ADD_BLOCK = 128
VMEM_BYTES = 67043328


def gelu(a):
    half = 0.5 * a
    return half + half * jnp.tanh(a * (C0 + C1 * (a * a)))


def cuts(total, step):
    return [(s, min(step, total - s)) for s in range(0, total, step)]


def ffn_kernel(parts, base, count_ref, *refs):
    xs, (win_hbm, wout_hbm), outs = refs[:parts], refs[parts:parts + 2], refs[parts + 2:2 * parts + 2]
    win_v, wout_v, h_v, x_v, o_v, wsem, xsem, osem = refs[2 * parts + 2:]
    ff, width = wout_v.shape
    ends = []
    total = 0
    for k in range(parts):
        total = total + count_ref[k]
        ends.append(total)
    load_in = pltpu.make_async_copy(win_hbm, win_v, wsem.at[0])
    load_out = pltpu.make_async_copy(wout_hbm, wout_v, wsem.at[1])
    load_in.start()
    load_out.start()

    def each_part(i, act):
        for k in range(parts):
            first = ends[k - 1] if k else 0

            @pl.when((i >= first) & (i < ends[k]))
            def _():
                act(k, pl.multiple_of((i - first) * BLOCK, BLOCK))

    def fetch(i, slot):
        each_part(i, lambda k, row: pltpu.make_async_copy(xs[k].at[pl.ds(base + row, BLOCK)], x_v.at[slot], xsem.at[slot]).start())

    def put(i, slot):
        each_part(i, lambda k, row: pltpu.make_async_copy(o_v.at[slot], outs[k].at[pl.ds(row, BLOCK)], osem.at[slot]).start())

    def wait_fetch(slot):
        pltpu.make_async_copy(xs[0].at[pl.ds(0, BLOCK)], x_v.at[slot], xsem.at[slot]).wait()

    def wait_put(slot):
        pltpu.make_async_copy(o_v.at[slot], outs[0].at[pl.ds(0, BLOCK)], osem.at[slot]).wait()

    fetch(0, 0)
    load_in.wait()

    @pl.when(total == 0)
    def _():
        load_out.wait()

    def step(i, carry):
        slot = lax.rem(i, 2)
        fetch(i + 1, 1 - slot)
        wait_fetch(slot)
        for st, sz in cuts(ff, 1280):
            a = jnp.dot(x_v[slot], win_v[:, st:st + sz], preferred_element_type=jnp.float32)
            h_v[:, st:st + sz] = gelu(a).astype(jnp.bfloat16)

        @pl.when(i == 0)
        def _():
            load_out.wait()

        @pl.when(i >= 2)
        def _():
            wait_put(slot)

        for st, sz in cuts(width, 768):
            o_v[slot, :, st:st + sz] = jnp.dot(h_v[...], wout_v[:, st:st + sz], preferred_element_type=jnp.float32).astype(jnp.bfloat16)
        put(i, slot)
        return carry

    lax.fori_loop(0, total, step, 0)

    @pl.when(total >= 1)
    def _():
        wait_put(lax.rem(total - 1, 2))

    @pl.when(total >= 2)
    def _():
        wait_put(lax.rem(total, 2))


def ffn(xs, counts, w_in, w_out, base=0, rows=None):
    parts = len(xs)
    width, ff = w_in.shape
    rows = rows or xs[0].shape[0]
    hbm = pl.BlockSpec(memory_space=pl.ANY)
    return pl.pallas_call(
        functools.partial(ffn_kernel, parts, base),
        in_specs=[pl.BlockSpec(memory_space=pltpu.SMEM)] + [hbm] * (parts + 2),
        out_specs=[hbm] * parts,
        out_shape=[jax.ShapeDtypeStruct((rows, width), x.dtype) for x in xs],
        scratch_shapes=[
            pltpu.VMEM((width, ff), jnp.bfloat16), pltpu.VMEM((ff, width), jnp.bfloat16), pltpu.VMEM((BLOCK, ff), jnp.bfloat16),
            pltpu.VMEM((2, BLOCK, width), jnp.bfloat16), pltpu.VMEM((2, BLOCK, width), jnp.bfloat16),
            pltpu.SemaphoreType.DMA((2,)), pltpu.SemaphoreType.DMA((2,)), pltpu.SemaphoreType.DMA((2,))],
        compiler_params=pltpu.CompilerParams(vmem_limit_bytes=VMEM_BYTES),
        cost_estimate=pl.CostEstimate(flops=2 * parts * rows * width * ff, bytes_accessed=4 * parts * rows * width + 4 * width * ff, transcendentals=0))(counts, *xs, w_in, w_out)


def add_kernel(parts, starts, final, count_ref, pair_ref, gate_ref, *refs):
    n_in = starts + 1
    ins, tables, (out,) = refs[:n_in], refs[n_in:n_in + parts], refs[n_in + parts:n_in + parts + 1]
    acc, rows_v, wide, buf_a, buf_b, rsem, asem, bsem = refs[n_in + parts + 1:]
    tokens, width = acc.shape
    block = rows_v.shape[1]
    cap = tables[0].shape[0]
    io = buf_a.shape[1]
    halves = cuts(width, (width // 256) * 128 or width)

    if starts:
        place = [(k, r) for k in range(starts) for r in range(0, ins[1 + k].shape[0], io)]
        n_io = tokens // io

        def load(i):
            a = pltpu.make_async_copy(ins[0].at[pl.ds(i * io, io)], buf_a.at[i % 2], asem.at[i % 2])
            b = pltpu.make_async_copy(ins[1 + place[i][0]].at[pl.ds(place[i][1], io)], buf_b.at[i % 2], bsem.at[i % 2])
            return a, b

        for c in load(0):
            c.start()
        for i in range(n_io):
            if i + 1 < n_io:
                for c in load(i + 1):
                    c.start()
            for c in load(i):
                c.wait()
            acc[pl.ds(i * io, io), :] = buf_a[i % 2].astype(jnp.float32) + buf_b[i % 2].astype(jnp.float32)
    else:
        whole = pltpu.make_async_copy(ins[0], acc, asem.at[0])
        whole.start()
        whole.wait()

    for k in range(parts):
        number = count_ref[k]
        blocks = (number + block - 1) // block

        def fetch(b, slot, k=k):
            return pltpu.make_async_copy(tables[k].at[pl.ds(pl.multiple_of(b * block, block), block)], rows_v.at[slot], rsem.at[slot])

        @pl.when(blocks > 0)
        def _(fetch=fetch):
            fetch(0, 0).start()

        def one_block(b, carry, k=k, fetch=fetch, blocks=blocks, number=number):
            slot = lax.rem(b, 2)

            @pl.when(b + 1 < blocks)
            def _():
                fetch(b + 1, 1 - slot).start()

            fetch(b, slot).wait()
            wide[...] = rows_v[slot].astype(jnp.float32)
            here = jnp.minimum(block, number - b * block)

            def some_rows(r, unroll):
                pairs = [pair_ref[k * cap + b * block + r + u] for u in range(unroll)]
                toks = [lax.shift_right_logical(p, 1) for p in pairs]
                gates = [gate_ref[p] for p in pairs]
                for st, sz in halves:
                    sums = [acc[pl.ds(t, 1), st:st + sz] + g * wide[pl.ds(r + u, 1), st:st + sz] for u, (t, g) in enumerate(zip(toks, gates))]
                    for t, s in zip(toks, sums):
                        acc[pl.ds(t, 1), st:st + sz] = s

            def four(q, c):
                some_rows(q * 4, 4)
                return c

            def single(r, c):
                some_rows(r, 1)
                return c

            lax.fori_loop(0, here // 4, four, 0)
            lax.fori_loop(here // 4 * 4, here, single, 0)
            return carry

        lax.fori_loop(0, blocks, one_block, 0)

    if final:
        n_io = tokens // io

        def store(i):
            return pltpu.make_async_copy(buf_a.at[i % 2], out.at[pl.ds(i * io, io)], asem.at[i % 2])

        for i in range(n_io):
            if i >= 2:
                store(i - 2).wait()
            buf_a[i % 2] = acc[pl.ds(i * io, io), :].astype(jnp.bfloat16)
            store(i).start()
        for i in range(max(n_io - 2, 0), n_io):
            store(i).wait()
    else:
        whole = pltpu.make_async_copy(acc, out, asem.at[0])
        whole.start()
        whole.wait()


def add_rows(ins, tables, counts, pairs, gates, tokens, final, io=256):
    width = tables[0].shape[1]
    starts = len(ins) - 1
    hbm = pl.BlockSpec(memory_space=pl.ANY)
    smem = pl.BlockSpec(memory_space=pltpu.SMEM)
    return pl.pallas_call(
        functools.partial(add_kernel, len(tables), starts, final),
        in_specs=[smem] * 3 + [hbm] * (len(ins) + len(tables)),
        out_specs=hbm,
        out_shape=jax.ShapeDtypeStruct((tokens, width), jnp.bfloat16 if final else jnp.float32),
        scratch_shapes=[
            pltpu.VMEM((tokens, width), jnp.float32), pltpu.VMEM((2, ADD_BLOCK, width), jnp.bfloat16), pltpu.VMEM((ADD_BLOCK, width), jnp.float32),
            pltpu.VMEM((2, io, width), jnp.bfloat16), pltpu.VMEM((2, io, width), jnp.bfloat16),
            pltpu.SemaphoreType.DMA((2,)), pltpu.SemaphoreType.DMA((2,)), pltpu.SemaphoreType.DMA((2,))],
        compiler_params=pltpu.CompilerParams(vmem_limit_bytes=VMEM_BYTES),
        cost_estimate=pl.CostEstimate(flops=60 * 1000 * 1000 * 1000, bytes_accessed=6 * tokens * width, transcendentals=0))(counts, pairs, gates, *ins, *tables)


def after(value, *others):
    return lax.optimization_barrier((value,) + others)[0]


def solution(mesh):
    group_size = mesh.shape['ep']

    def swap(x, bits):
        return lax.ppermute(x, 'ep', [(i, i ^ bits) for i in range(group_size)])

    def layer(tok_x, route_ids, route_gate, w_in, w_out, shared_in, shared_out):
        tokens, _ = tok_x.shape
        top_k = route_ids.shape[1]
        experts = group_size
        capacity = tokens * group_size * top_k // experts
        local_cap = 2 * tokens * top_k // experts
        half = tokens // 2
        me = lax.axis_index('ep')
        partner = jnp.bitwise_xor(me, jnp.arange(experts, dtype=jnp.int32))

        flat_ids = route_ids.reshape(-1)
        onehot = (flat_ids[:, None] == jnp.arange(experts, dtype=jnp.int32)[None, :]).astype(jnp.int32)
        running = jnp.cumsum(onehot, axis=0)
        rank = jnp.sum(running * onehot, axis=1) - 1
        counts = running[-1]
        pair_number = jnp.arange(tokens * top_k, dtype=jnp.int32)
        lists = jnp.zeros((experts * local_cap,), jnp.int32).at[flat_ids * local_cap + rank].set(pair_number)
        lists = lists.reshape(experts, local_cap)
        notes = jnp.concatenate([lists, jnp.broadcast_to(jnp.pad(counts, (0, 128 - experts))[None, :], (experts, 128))], axis=1)
        core_note = lax.dynamic_index_in_dim(notes, jnp.bitwise_xor(me, 1), 0, keepdims=True)
        core_note = swap(core_note, 1)[0]
        notes = lax.all_to_all(notes, 'ep', 0, 0, tiled=True)
        home_pairs = lists[partner]
        gates = route_gate.reshape(-1)

        from_core = swap(tok_x, 1)
        from_x = swap(tok_x, 2)
        from_y = swap(tok_x, 4)

        home = [None] * experts

        def expert(group, sources, previous, toks, numbers):
            rows = [x[toks[s]] for x, s in zip(sources, group)]
            number = after(jnp.stack([numbers[s] for s in group]), previous)
            outs = ffn(rows, number, w_in[0], w_out[0])
            for s, out in zip(group, outs):
                home[s] = swap(out, s) if s else out
            return outs[0]

        own_list = lax.dynamic_index_in_dim(lists, me, 0, keepdims=False)
        own_count = lax.dynamic_index_in_dim(counts, me, 0, keepdims=False)
        core_count = lax.dynamic_index_in_dim(core_note, local_cap + me, 0, keepdims=False)
        core_toks = (own_list // top_k, core_note[:local_cap] // top_k)
        core_numbers = ((own_count + BLOCK - 1) // BLOCK, (core_count + BLOCK - 1) // BLOCK)
        first_rows = tokens * 3 // 8
        rest_rows = tokens - first_rows
        last = expert((0, 1), (tok_x, from_core), counts, core_toks, core_numbers)
        shared_a, = ffn([tok_x], after(jnp.full((1,), first_rows // BLOCK, jnp.int32), last), shared_in, shared_out, 0, first_rows)
        from_x, from_y, notes = lax.optimization_barrier((from_x, from_y, notes, shared_a))[:3]

        all_counts = notes[:, local_cap:local_cap + experts]
        offset = jnp.cumsum(all_counts, axis=0) - all_counts
        kept = jnp.clip(capacity - offset, 0, all_counts)
        kept_out = lax.dynamic_index_in_dim(kept, me, 0, keepdims=False)[partner]
        kept_here = lax.dynamic_index_in_dim(kept, me, 1, keepdims=False)[partner]
        here_toks = notes[partner][:, :local_cap] // top_k
        block_counts = (kept_here + BLOCK - 1) // BLOCK

        part_x, part_y = from_x[:half], from_y[half:]
        diag_a = swap(part_x, 4)
        diag_b = swap(part_y, 2)
        core_x = swap(from_x, 1)
        core_y = swap(from_y, 1)
        last = expert((2, 4), (from_x, from_y), shared_a, here_toks, block_counts)
        diag_a, diag_b = after(diag_a, last), after(diag_b, last)
        diag = jnp.concatenate([diag_a, diag_b], axis=0)
        core_diag = swap(diag, 1)
        last = expert((3, 5), (core_x, core_y), last, here_toks, block_counts)
        last = expert((6,), (diag,), last, here_toks, block_counts)
        last = expert((7,), (core_diag,), last, here_toks, block_counts)
        shared_b, = ffn([tok_x], after(jnp.full((1,), rest_rows // BLOCK, jnp.int32), last), shared_in, shared_out, first_rows, rest_rows)

        def add(ins, classes, final):
            return add_rows(ins, [home[s] for s in classes], jnp.stack([kept_out[s] for s in classes]),
                            jnp.concatenate([home_pairs[s] for s in classes]), gates, tokens, final)

        total = add([tok_x, shared_a, shared_b], (0, 1, 2, 4), False)
        return add([total], (3, 5, 6, 7), True)

    row_spec = P(('dp', 'ep'), None)
    expert_spec = P('ep', None, None)
    whole_spec = P(None, None)
    return jax.shard_map(layer, mesh=mesh, in_specs=(row_spec, row_spec, row_spec, expert_spec, expert_spec, whole_spec, whole_spec), out_specs=row_spec, check_vma=False)
```
